32 devices in a mesh: rep: 1, dp: 32 (over x, y, z, core).
Axes of the slice: x: 2, y: 2, z: 4, core: 2. Of those that a mesh axis runs over, the one named last changes fastest.
Arguments:
- x: bfloat16 [32, 2048, 768], P(('rep', 'dp'))
- dy: bfloat16 [32, 2048, 768], P(('rep', 'dp'))
- w_gate: bfloat16 [2, 768, 3072], replicated
- w_up: bfloat16 [2, 768, 3072], replicated
- w_down: bfloat16 [2, 3072, 768], replicated
- m_w_gate: float32 [2, 768, 3072], replicated
- m_w_up: float32 [2, 768, 3072], replicated
- m_w_down: float32 [2, 3072, 768], replicated
- v_w_gate: float32 [2, 768, 3072], replicated
- v_w_up: float32 [2, 768, 3072], replicated
- v_w_down: float32 [2, 3072, 768], replicated
Outputs:
- output 1: bfloat16 [2, 768, 3072], P('rep')
- output 2: bfloat16 [2, 768, 3072], P('rep')
- output 3: bfloat16 [2, 3072, 768], P('rep')
- output 4: float32 [2, 768, 3072], P('rep')
- output 5: float32 [2, 768, 3072], P('rep')
- output 6: float32 [2, 3072, 768], P('rep')
- output 7: float32 [2, 768, 3072], P('rep')
- output 8: float32 [2, 768, 3072], P('rep')
- output 9: float32 [2, 3072, 768], P('rep')
All inputs are finite; a program needn't handle non-finite values.
Results may differ from the reference program's by a relative error of at most 0.022.
Values are sent between devices in bfloat16 or wider.
A program may use at most 2.5 GiB of HBM per device.

```python
import jax
import jax.numpy as jnp
from jax import lax

SEQUENCES = 32
TOKENS = 2048
D = 768
FF = 3072
LAYERS = 2
NAMES = ("w_gate", "w_up", "w_down")
SHAPES = {"w_gate": (LAYERS, D, FF), "w_up": (LAYERS, D, FF), "w_down": (LAYERS, FF, D)}


def bump(key, n, height):
    away = (jnp.arange(n, dtype=jnp.int32) - jax.random.randint(key, (), 0, n, jnp.int32)) % n
    return jnp.where(away < n // 8, height, 1.0)


def together(key, own, strength):
    shared = jax.random.normal(key, own.shape[1:], jnp.float32)
    return (own + strength * shared) * lax.rsqrt(1 + strength * strength)


def setup_inputs(seed: int = 0, part: int = 0) -> dict:
    kx, kdy, ka, kb, kz, kf, kh, kl, *keys = jax.random.split(jax.random.key(seed), 8 + 3 * len(NAMES))
    kx, kdy, ka, kb = (jax.random.fold_in(k, part) for k in (kx, kdy, ka, kb))
    kw, km, kv = (keys[i::3] for i in range(3))
    shape = (SEQUENCES, TOKENS, D)
    much_x, much_dy = jax.random.uniform(kz, (2,), jnp.float32, 0.0, 1.0)
    loud = 2.0 ** jax.random.uniform(jax.random.fold_in(kz, 1), (), jnp.float32, -1.0, 2.0)
    layers = 2.0 ** jax.random.uniform(kl, (LAYERS, 1, 1), jnp.float32, -1.0, 1.0)
    x = together(ka, jax.random.normal(kx, shape, jnp.float32), much_x) * bump(kf, D, 4.0)
    dy = together(kb, jax.random.normal(kdy, shape, jnp.float32), much_dy)
    drawn = {"x": x.astype(jnp.bfloat16), "dy": (loud * dy * (SEQUENCES * TOKENS) ** -0.5).astype(jnp.bfloat16)}
    for key, name in zip(kw, NAMES, strict=True):
        w = jax.random.normal(key, SHAPES[name], jnp.float32) * SHAPES[name][1] ** -0.5
        drawn[name] = (w * {"w_gate": 1.0, "w_up": bump(kh, FF, 4.0), "w_down": layers}[name]).astype(jnp.bfloat16)
    for key, name in zip(km, NAMES, strict=True):
        drawn[f"m_{name}"] = 0.1 * jax.random.normal(key, SHAPES[name], jnp.float32)
    for key, name in zip(kv, NAMES, strict=True):
        drawn[f"v_{name}"] = jax.random.uniform(key, SHAPES[name], jnp.float32, 0.005, 0.015)
    return drawn


def matmul(a, w):
    return jnp.dot(a, w, preferred_element_type=jnp.float32).astype(jnp.bfloat16)


def normed(h):
    wide = h.astype(jnp.float32)
    scale = lax.rsqrt(jnp.mean(wide**2, -1, keepdims=True) + 1e-6)
    return (wide * scale).astype(jnp.bfloat16)


def layer(h, w):
    a = normed(h)
    gate = jnp.dot(a, w["w_gate"], preferred_element_type=jnp.float32)
    up = jnp.dot(a, w["w_up"], preferred_element_type=jnp.float32)
    return h + matmul((jax.nn.silu(gate) * up).astype(jnp.bfloat16), w["w_down"])


def adamw(w, m, v, g):
    m = 0.9 * m + 0.1 * g
    v = 0.95 * v + 0.05 * g * g
    step = m * lax.rsqrt(v + 1e-8) + 0.1 * w
    return (w - 0.02 * step).astype(jnp.bfloat16), m, v


def clipped(gradients, sum_of_squares, count):
    factor = jnp.minimum(1.0, 0.5 * lax.rsqrt(sum_of_squares / count + 1e-30))
    return [g * factor for g in gradients]


def stack(weights, h):
    return lax.scan(lambda h, w: (layer(h, w), None), h, weights)[0]


def reference(x, dy, w_gate, w_up, w_down, m_w_gate, m_w_up, m_w_down, v_w_gate, v_w_up, v_w_down):
    weights = dict(zip(NAMES, (w_gate, w_up, w_down), strict=True))

    def take(so_far, sequence):
        h, by_y = sequence
        _, back = jax.vjp(lambda w: stack(w, h), weights)
        return jax.tree.map(lambda total, term: total + term.astype(jnp.float32), so_far, back(by_y)[0]), None

    none_yet = {name: jnp.zeros(w.shape, jnp.float32) for name, w in weights.items()}
    by_weights, _ = lax.scan(take, none_yet, (x, dy))
    gradients = [by_weights[name].astype(jnp.bfloat16).astype(jnp.float32) for name in NAMES]
    gradients = clipped(gradients, sum(jnp.sum(g * g) for g in gradients), sum(g.size for g in gradients))
    new = [
        adamw(w.astype(jnp.float32), m, v, g)
        for w, m, v, g in zip((w_gate, w_up, w_down), (m_w_gate, m_w_up, m_w_down), (v_w_gate, v_w_up, v_w_down), gradients, strict=True)
    ]
    return tuple(one[which] for which in range(3) for one in new)
```

```python
import functools

import jax
import jax.numpy as jnp
from jax import lax
from jax.experimental import pallas as pl
from jax.experimental.pallas import tpu as pltpu
from jax.sharding import PartitionSpec as P

D, FF = 768, 3072
MESH = pl.DeviceIdType.MESH
HALF, COLOR, FIRST, SECOND = 384, 192, 96, 48
ZS = 4
WIDE, TALL = 512, 192
VMEM_LIMIT = 63 * 1024 * 1024
F32, BF16 = jnp.float32, jnp.bfloat16


OPT_STEPS = 12


def adamw_kernel(count, square_ref, *refs):
    factor = jnp.minimum(1.0, 0.5 * lax.rsqrt(jnp.sum(square_ref[...], keepdims=True) / count + 1e-30))
    for k in range(3):
        w, m, v, g, new_w, new_m, new_v = (refs[k + 3 * i] for i in range(7))

        @pl.when(pl.program_id(0) // OPT_STEPS == k)
        def _():
            rows = 128 if k == 2 else 16

            def body(r, _):
                at = pl.ds(pl.multiple_of(r * rows, rows), rows)
                wide = (g[:, at].astype(F32).T if k == 2 else g[at].astype(F32)) * factor
                mm = 0.9 * m[at] + 0.1 * wide
                vv = 0.95 * v[at] + 0.05 * wide * wide
                ww = w[at].astype(F32)
                new_m[at], new_v[at] = mm, vv
                new_w[at] = (ww - 0.02 * (mm * lax.rsqrt(vv + 1e-8) + 0.1 * ww)).astype(BF16)
                return 0

            lax.fori_loop(0, w.shape[0] // rows, body, 0)


def adamw(square, *arrays):
    def spec(k):
        if k == 11:
            turns, step = OPT_STEPS // 2, lambda t: jnp.clip(t - 2 * OPT_STEPS, 0, OPT_STEPS - 1)
            return pl.BlockSpec((D, FF // turns), lambda t: (step(t) // turns, step(t) % turns))
        rows, columns = arrays[k % 3].shape
        return pl.BlockSpec((rows // OPT_STEPS, columns), lambda t: (jnp.clip(t - OPT_STEPS * (k % 3), 0, OPT_STEPS - 1), 0))

    specs = [spec(k) for k in range(12)]
    like = lambda k, dtype: jax.ShapeDtypeStruct(arrays[k].shape, dtype)
    return pl.pallas_call(
        functools.partial(adamw_kernel, sum(w.size for w in arrays[:3])),
        grid=(3 * OPT_STEPS,),
        in_specs=[pl.BlockSpec((8, 128), lambda t: (0, 0))] + specs,
        out_specs=specs[:9],
        out_shape=[like(k, BF16) for k in range(3)] + [like(k, F32) for k in range(3)] * 2,
        compiler_params=pltpu.CompilerParams(dimension_semantics=("arbitrary",), vmem_limit_bytes=VMEM_LIMIT),
        name="adamw",
    )(square, *arrays)


TT, FC = 256, 768


def dot(a, b, dims=((1,), (0,))):
    return lax.dot_general(a, b, (dims, ((), ())), preferred_element_type=F32)


def rms_scale(wide):
    return lax.rsqrt(jnp.mean(wide * wide, -1, keepdims=True) + 1e-6)


def tokens_kernel(x_ref, dy_ref, wg_hbm, wu_hbm, wd_hbm, a0_ref, a1_ref, dy_out, dh_ref, act0, dg0, du0, act1, dg1, du1, wg, wu, wd, keep_g, keep_u, sem):
    step = pl.program_id(0)
    loads = [
        pltpu.make_async_copy(hbm.at[l], vmem.at[l], sem.at[l * 3 + k])
        for l in range(2)
        for k, (hbm, vmem) in enumerate(((wg_hbm, wg), (wu_hbm, wu), (wd_hbm, wd)))
    ]

    @pl.when(step == 0)
    def _():
        for load in loads:
            load.start()

    def ready(*which):
        @pl.when(step == 0)
        def _():
            for k in which:
                loads[k].wait()

    h0 = x_ref[...].astype(F32)
    a0 = (h0 * rms_scale(h0)).astype(BF16)
    a0_ref[...] = a0.T
    ready(0, 1, 2)
    total = jnp.zeros((TT, D), F32)
    for j in range(FF // FC):
        at = slice(j * FC, (j + 1) * FC)
        gate, up = dot(a0, wg[0, :, at]), dot(a0, wu[0, :, at])
        keep_g[:, at], keep_u[:, at] = gate, up
        act = (gate * jax.nn.sigmoid(gate) * up).astype(BF16)
        act0[:, at] = act
        total = total + dot(act, wd[0, at, :])
    h1 = (h0 + total.astype(BF16).astype(F32)).astype(BF16).astype(F32)
    scale1 = rms_scale(h1)
    a1 = (h1 * scale1).astype(BF16)
    a1_ref[...] = a1.T
    ready(3, 4, 5)

    def back(dact, gate, up):
        dact = dact.astype(BF16).astype(F32)
        sig = jax.nn.sigmoid(gate)
        silu = gate * sig
        return silu * up, dact * up * (sig + silu * (1.0 - sig)), dact * silu

    dy = dy_ref[...]
    dy_out[...] = dy.T
    by_gate, by_up = jnp.zeros((TT, D), F32), jnp.zeros((TT, D), F32)
    nt = ((1,), (1,))
    for j in range(FF // FC):
        at = slice(j * FC, (j + 1) * FC)
        gate, up = dot(a1, wg[1, :, at]), dot(a1, wu[1, :, at])
        act, dg, du = back(dot(dy, wd[1, at, :], nt), gate, up)
        dg, du = dg.astype(BF16), du.astype(BF16)
        act1[:, at], dg1[:, at], du1[:, at] = act.astype(BF16), dg, du
        by_gate = by_gate + dot(dg, wg[1, :, at], nt)
        by_up = by_up + dot(du, wu[1, :, at], nt)
    da = (by_gate.astype(BF16).astype(F32) + by_up.astype(BF16).astype(F32)).astype(BF16).astype(F32)
    along = jnp.sum(da * h1, -1, keepdims=True)
    dwide = da * scale1 - h1 * (scale1 * scale1 * scale1 * along * (1.0 / D))
    dh = (dy.astype(F32) + dwide.astype(BF16).astype(F32)).astype(BF16)
    dh_ref[...] = dh.T
    for j in range(FF // FC):
        at = slice(j * FC, (j + 1) * FC)
        _, dg, du = back(dot(dh, wd[0, at, :], nt), keep_g[:, at], keep_u[:, at])
        dg0[:, at], du0[:, at] = dg.astype(BF16), du.astype(BF16)


def tokens(x, dy, wg, wu, wd):
    n = x.shape[0]
    narrow = pl.BlockSpec((TT, D), lambda t: (t, 0))
    turned = pl.BlockSpec((D, TT), lambda t: (0, t))
    wide = pl.BlockSpec((TT, FF), lambda t: (t, 0))
    anywhere = pl.BlockSpec(memory_space=pl.ANY)
    big = jax.ShapeDtypeStruct((n, FF), BF16)
    return pl.pallas_call(
        tokens_kernel,
        grid=(n // TT,),
        in_specs=[narrow, narrow, anywhere, anywhere, anywhere],
        out_specs=[turned] * 4 + [wide] * 6,
        out_shape=[jax.ShapeDtypeStruct((D, n), BF16)] * 4 + [big] * 6,
        scratch_shapes=[
            pltpu.VMEM((2, D, FF), BF16),
            pltpu.VMEM((2, D, FF), BF16),
            pltpu.VMEM((2, FF, D), BF16),
            pltpu.VMEM((TT, FF), F32),
            pltpu.VMEM((TT, FF), F32),
            pltpu.SemaphoreType.DMA((6,)),
        ],
        compiler_params=pltpu.CompilerParams(dimension_semantics=("arbitrary",), vmem_limit_bytes=VMEM_LIMIT),
        name="tokens",
    )(x, dy, wg, wu, wd)


def part(ref, row, rows, block=0, blocks=ZS):
    return ref.at[pl.ds(pl.multiple_of(row, 16), rows), pl.ds(pl.multiple_of(block * D, D), blocks * D)]


def hold(rows, blocks=ZS):
    return pltpu.VMEM((rows, blocks * D), BF16)


def slabs(rows, blocks, body):
    n = rows // 16
    lax.fori_loop(0, n * blocks, lambda i, _: (body(lax.rem(i, n) * 16, i // n), 0)[1], 0)


def group_sum_kernel(layers_of, slots, smalls_key, *refs):
    count = len(slots)
    smalls, bigs, refs = refs[:count], refs[count : 2 * count], refs[2 * count :]
    outs, norm_out, refs = refs[:3], refs[3], refs[4:]
    own, r0, r1, r2, r3, r4, fin, refs = *(refs[i * count : (i + 1) * count] for i in range(7)), refs[7 * count :]
    square, told, send, recv, local, norm_send, norm_recv, staged, small, block, load_sem = refs
    full = [outs[slots[n]].at[layers_of[n]] for n in range(count)]

    i = lax.axis_index("dp")
    c, z, y, x = lax.rem(i, 2), lax.rem(i // 2, 4), lax.rem(i // 8, 2), i // 16

    def device(x, y, z, c):
        return {"dp": ((x * 2 + y) * 4 + z) * 2 + c}

    partner = device(x, y, z, 1 - c)
    by_x, by_y = device(1 - x, y, z, c), device(x, 1 - y, z, c)
    z0, z1 = lax.rem(z, 2), z // 2
    by_z0, by_z1 = device(x, y, z + 1 - 2 * z0, c), device(x, y, lax.rem(z + 2, 4), c)
    halves = ((x, z0, y, z1), (y, z0, x, z1))
    others = ((by_x, by_z0, by_y, by_z1), (by_y, by_z0, by_x, by_z1))

    def remote(n, slot, src, dst, to):
        return pltpu.make_async_remote_copy(
            src_ref=src, dst_ref=dst, send_sem=send.at[n, slot], recv_sem=recv.at[n, slot], device_id=to, device_id_type=MESH
        )

    def row_of(k, depth):
        f, g = halves[k][:2]
        return k * COLOR + (f * FIRST if depth >= 1 else 0) + (g * SECOND if depth >= 2 else 0)

    def small_load(n):
        return pltpu.make_async_copy(smalls[n], small.at[small_slot[n]], load_sem.at[2 + small_slot[n]])

    small_slot, new_small = [0], [True]
    for n in range(1, count):
        new_small.append(smalls_key[n] != smalls_key[n - 1])
        small_slot.append(small_slot[-1] ^ new_small[-1])

    def block_load(n, j, slot):
        at = pl.ds(pl.multiple_of(j * WIDE, WIDE), WIDE)
        return pltpu.make_async_copy(bigs[n].at[:, at], block.at[slot], load_sem.at[slot])

    def compute(n, mine):
        into = own[n] if mine else staged[n % 2]
        follows = n + mine
        if not mine:
            if new_small[n]:
                small_load(n).wait()
            if n >= 2:
                state0[n - 2].wait_send()
        turns = FF // WIDE // 2

        def body(p, _):
            for slot in range(2):
                j = 2 * p + slot
                block_load(n, j, slot).wait()
                for q in range(0, HALF, TALL):
                    rows = pl.ds(pl.multiple_of((c if mine else 1 - c) * HALF + q, TALL), TALL)
                    columns = pl.ds(pl.multiple_of(j * WIDE, WIDE), WIDE)
                    into[q : q + TALL, columns] = dot(small[small_slot[n], rows], block[slot]).astype(BF16)

                @pl.when(p < turns - 1)
                def _():
                    block_load(n, j + 2, slot).start()

                if follows < count:

                    @pl.when(p == turns - 1)
                    def _():
                        block_load(follows, slot, slot).start()

            return 0

        lax.fori_loop(0, turns, body, 0)
        if not mine and n + 1 < count and new_small[n + 1]:
            small_load(n + 1).start()

    state0 = {}

    def start0(n):
        theirs = remote(n, 0, staged[n % 2], r0[n], partner)
        theirs.start()
        state0[n] = theirs
        return [], [theirs]

    def at16(ref, row, b):
        return ref.at[pl.ds(pl.multiple_of(row, 16), 16), pl.ds(pl.multiple_of(b * D, D), D)]

    def partial(n, k, row, b, depth):
        s = halves[k][2]
        terms = [(own, row, b), (r0, row, b)]
        if depth >= 1:
            terms.append((r1, row - row_of(k, 1) + k * FIRST, b))
        if depth >= 2:
            terms.append((r2, row - row_of(k, 2) + k * SECOND, b))
        if depth >= 3:
            terms.append((r3, row - row_of(k, 2) + k * SECOND, b - 2 * s))
        if depth >= 4:
            terms.append((r4, row - row_of(k, 2) + k * SECOND, 0))
        value = None
        for ref, at, block_ in terms:
            term = at16(ref[n], at, block_)[...].astype(F32)
            value = term if value is None else value + term
        return value

    def send_half(step):
        def start(n):
            out = []
            for k in range(2):
                f, g, s, q = halves[k]
                if step == 1:
                    row, rows, b, blocks, into, to_row = k * COLOR + (1 - f) * FIRST, FIRST, 0, ZS, r1, k * FIRST
                elif step == 2:
                    row, rows, b, blocks, into, to_row = row_of(k, 1) + (1 - g) * SECOND, SECOND, 0, ZS, r2, k * SECOND
                elif step == 3:
                    row, rows, b, blocks, into, to_row = row_of(k, 2), SECOND, 2 * (1 - s), 2, r3, k * SECOND
                else:
                    row, rows, b, blocks, into, to_row = row_of(k, 2), SECOND, 2 * s + 1 - q, 1, r4, k * SECOND

                def body(r, bb):
                    at16(own[n], row + r, b + bb)[...] = partial(n, k, row + r, b + bb, step - 1).astype(BF16)

                slabs(rows, blocks, body)
                src = part(own[n], row, rows, b, blocks)
                out.append(remote(n, 2 * step - 1 + k, src, part(into[n], to_row, rows, 0, blocks), others[k][step - 1]))
                out[-1].start()
            return [], out

        return start

    def place(n, k, depth):
        f, g, s, q = halves[k]
        row, rows = (row_of(k, 2), SECOND) if depth >= 2 else (row_of(k, 1), FIRST)
        b, blocks = {4: (2 * s + q, 1), 3: (2 * s, 2)}.get(depth, (0, ZS))
        return part(full[n], c * HALF + row, rows, b, blocks)

    def finish(n):
        here, out = [], []
        for k in range(2):
            f, g, s, q = halves[k]

            def body(r, _):
                value = partial(n, k, row_of(k, 2) + r, 2 * s + q, 4).astype(BF16)
                at16(fin[n], k * SECOND + r, 0)[...] = value
                value = value.astype(F32)
                value = value * value
                pieces = [value[8 * a : 8 * a + 8, 128 * b : 128 * b + 128] for a in range(2) for b in range(D // 128)]
                square[...] += sum(pieces[1:], pieces[0])

            slabs(SECOND, 1, body)
            src = part(fin[n], k * SECOND, SECOND, 0, 1)
            here.append(pltpu.make_async_copy(src, place(n, k, 4), local.at[n, k]))
            here[-1].start()
            out.append(remote(n, 9 + k, src, place(n, k, 4), others[k][3]))
            out[-1].start()
        return here, out

    def pass_on(step):
        def start(n):
            out = []
            for k in range(2):
                where = place(n, k, step)
                out.append(remote(n, 17 - 2 * step + k, where, where, others[k][step - 1]))
                out[-1].start()
            return [], out

        return start

    def last(n):
        where = part(full[n], c * HALF, HALF)
        out = remote(n, 17, where, where, partner)
        out.start()
        return [], [out]

    stages = (start0, *(send_half(s) for s in (1, 2, 3, 4)), finish, *(pass_on(s) for s in (3, 2, 1)), last)
    state, sent = {}, []

    def run(n, stage):
        if stage:
            here, out = state[n]
            for copy in here:
                copy.wait()
            for copy in out:
                copy.wait_recv()
        if stage < len(stages):
            state[n] = stages[stage](n)
            if stage:
                sent.extend(state[n][1])

    square[...] = jnp.zeros_like(square)
    small_load(0).start()
    for which in range(2):
        block_load(0, which, which).start()
    exchange = [partner, by_x, by_y, by_z0, by_z1]
    norm_step, pending = 0, None

    def norm_round():
        nonlocal norm_step, pending
        if pending is not None:
            pending.wait()
            told[2 * norm_step + 2] = told[2 * norm_step] + told[2 * norm_step + 1]
            norm_step += 1
            pending = None
        if norm_step < len(exchange):
            pending = pltpu.make_async_remote_copy(
                src_ref=told.at[2 * norm_step],
                dst_ref=told.at[2 * norm_step + 1],
                send_sem=norm_send.at[norm_step],
                recv_sem=norm_recv.at[norm_step],
                device_id=exchange[norm_step],
                device_id_type=MESH,
            )
            pending.start()

    halves_done = finished = 0
    for n, stage in ORDER:
        if stage is None:
            compute(halves_done // 2, halves_done % 2)
            if halves_done % 2 == 0:
                run(halves_done // 2, 0)
            halves_done += 1
            continue
        run(n, stage)
        finished += stage == 5
        if finished == count:
            if stage == 5:
                told[0] = square[...]
            norm_round()
    while norm_step < len(exchange):
        norm_round()
    norm_out[...] = told[2 * len(exchange)]
    for n in range(count):
        run(n, len(stages))
    for copy in sent + [state0[n] for n in range(count - 2, count)]:
        copy.wait_send()


ORDER = (
    (None, None), (None, None), (0, 1), (None, None), (None, None), (0, 2), (1, 1), (None, None), (None, None), (0, 3),
    (1, 2), (2, 1), (None, None), (0, 4), (None, None), (0, 5), (1, 3), (2, 2), (3, 1), (None, None),
    (1, 4), (0, 6), (None, None), (2, 3), (3, 2), (1, 5), (4, 1), (0, 7), (None, None), (2, 4),
    (None, None), (3, 3), (4, 2), (5, 1), (1, 6), (3, 4), (2, 5), (5, 2), (1, 7), (4, 3),
    (3, 5), (4, 4), (2, 6), (2, 7), (5, 3), (0, 8), (5, 4), (1, 8), (3, 6), (4, 5),
    (0, 9), (1, 9), (2, 8), (5, 5), (3, 7), (4, 6), (5, 6), (2, 9), (4, 7), (5, 7),
    (3, 8), (4, 8), (3, 9), (5, 8), (4, 9), (5, 9),
)


def group_sum(pairs, layers_of, slots, smalls_key):
    count = len(pairs)
    scratch = []
    for one in (
        hold(HALF),
        hold(HALF),
        hold(2 * FIRST),
        hold(2 * SECOND),
        hold(2 * SECOND, 2),
        hold(2 * SECOND, 1),
        hold(2 * SECOND, 1),
    ):
        scratch += [one] * count
    dma = pltpu.SemaphoreType.DMA
    scratch += [
        pltpu.VMEM((8, 128), F32),
        pltpu.VMEM((11, 8, 128), F32),
        dma((count, 18)),
        dma((count, 18)),
        dma((count, 2)),
        dma((5,)),
        dma((5,)),
        [hold(HALF)] * 2,
        pltpu.VMEM((2, *pairs[0][0].shape), BF16),
        pltpu.VMEM((2, pairs[0][1].shape[0], WIDE), BF16),
        dma((4,)),
    ]
    out = pl.pallas_call(
        functools.partial(group_sum_kernel, layers_of, slots, smalls_key),
        out_shape=(
            jax.ShapeDtypeStruct((2, D, FF), BF16),
            jax.ShapeDtypeStruct((2, D, FF), BF16),
            jax.ShapeDtypeStruct((2, D, FF), BF16),
            jax.ShapeDtypeStruct((8, 128), F32),
        ),
        in_specs=[pl.BlockSpec(memory_space=pl.ANY)] * (2 * count),
        out_specs=(pl.BlockSpec(memory_space=pl.ANY),) * 3 + (pl.BlockSpec(memory_space=pltpu.VMEM),),
        scratch_shapes=scratch,
        compiler_params=pltpu.CompilerParams(has_side_effects=True, vmem_limit_bytes=VMEM_LIMIT),
        name="group_sum",
    )(*[small for small, _ in pairs], *[big for _, big in pairs])
    return out


def solution(mesh):
    def step(x, dy, *arrays):
        weights, m, v = (arrays[i : i + 3] for i in (0, 3, 6))
        a0, a1, dy_t, dh_t, act0, dg0, du0, act1, dg1, du1 = tokens(x[0], dy[0], *weights)
        pairs = ((dy_t, act1), (a1, dg1), (a1, du1), (dh_t, act0), (a0, dg0), (a0, du0))
        *summed, square = group_sum(pairs, (1, 1, 1, 0, 0, 0), (2, 0, 1) * 2, (0, 1, 1, 2, 3, 3))
        flat = [one.reshape(-1, one.shape[-1]) for one in (*weights, *m, *v, *summed)]
        return tuple(one.reshape(weights[k % 3].shape) for k, one in enumerate(adamw(square, *flat)))

    return jax.shard_map(
        step,
        mesh=mesh,
        in_specs=(P(("rep", "dp"), None, None),) * 2 + (P(None, None, None),) * 9,
        out_specs=(P("rep", None, None),) * 9,
        check_vma=False,
    )
```
